128 devices in a mesh: pb: 2 (over z_lo), row: 16 (over x, y), col: 4 (over z_hi, core).
Axes of the slice: x: 4, y: 4, z: 4 (z_hi: 2, z_lo: 2; z = z_hi * 2 + z_lo), core: 2. Of those that a mesh axis runs over, the one named last changes fastest.
Arguments:
- chol: bfloat16 [256, 1344, 1344], P('pb', 'row', 'col'), may hold values from -0.29882812 to 0.29882812
- amplitudes: bfloat16 [144, 1200], P(None, 'row'), may hold values from -0.59765625 to 0.59765625
Outputs:
- dressed: bfloat16 [256, 1344, 1344], P(('pb', 'row', 'col'))
- fock: float32 [1344, 1344], P('row', 'col')
The draws below stay inside these ranges and needn't reach their ends.
All inputs are finite; a program needn't handle non-finite values.
Results may differ from the reference program's by a relative error of at most 0.02.
Values may be sent and summed in bfloat16 or wider, within the bound.
No kernel may reach another device: no remote copies, remote signals or barrier semaphores. Data moves between devices by JAX's collectives and lax.ppermute only.
A program may use at most 128 MiB of HBM per device.

```python
import jax
import jax.numpy as jnp
from jax import lax

NG = 16
OCC = 144
VIR = 1200
OG = 9
VG = 75
SH = 84
NORB = 1344
Q = 256
N_ROW = 16


def levels(rng, dims, cuts, smallest, high):
    def one(dim, shards_of):
        steps = jax.random.uniform(jax.random.fold_in(jax.random.fold_in(rng, 6), dim), (shards_of,), jnp.float32, smallest / len(cuts), high / len(cuts))
        return jnp.repeat(jnp.exp(steps), dims[dim] // shards_of).reshape((-1,) + (1,) * (len(dims) - dim - 1))

    gain = one(*cuts[0])
    for cut in cuts[1:]:
        gain = gain * one(*cut)
    return gain


def normal_values(own_key, extent, scale, most, shards=(), held_as=jnp.bfloat16):
    values = scale * jax.random.normal(own_key, extent, jnp.float32)
    if shards:
        values = values * levels(own_key, extent, shards, -0.22, 0.18)
    return jnp.clip(values, -most, most).astype(held_as)


def setup_inputs(seed: int = 0) -> dict:
    splits = jax.random.split(jax.random.key(seed), 3)
    return {
        "chol": normal_values(splits[0], (Q, NORB, NORB), 0.05, 0.29882812, ((0, 2), (1, 16), (2, 4))),
        "amplitudes": normal_values(splits[1], (OCC, VIR), 0.1, 0.59765625, ((1, 16),)),
    }


block_vectors = 16


def reference(chol, amplitudes):
    amp_float = amplitudes.astype(jnp.float32)
    span = (NG // N_ROW) * VG
    amp_blocks = jnp.moveaxis(amp_float.reshape(OCC, N_ROW, span), 1, 0)

    def one_block(total, piece):
        layered = piece.reshape(block_vectors, NG, SH, NORB)
        occ_rows = layered[:, :, :OG, :].astype(jnp.float32)
        vir_rows = layered[:, :, OG:, :].astype(jnp.float32).reshape(block_vectors, N_ROW, span, NORB)
        vir_blocks = jnp.moveaxis(vir_rows, 1, 0)

        def add_block(acc, pair):
            amp_part, rows_part = pair
            term = jnp.einsum("ia,qab->qib", amp_part, rows_part)
            term = lax.optimization_barrier(term.astype(jnp.bfloat16))
            return acc + term.astype(jnp.float32), None

        shift, unused = lax.scan(add_block, jnp.zeros((block_vectors, OCC, NORB), jnp.float32), (amp_blocks, vir_blocks))
        occ_new = occ_rows - shift.reshape(block_vectors, NG, OG, NORB)
        primed = jnp.concatenate([occ_new, layered[:, :, OG:, :].astype(jnp.float32)], axis=2)
        primed = primed.reshape(block_vectors, NORB, NORB).astype(jnp.bfloat16)
        columns = primed.reshape(block_vectors, NORB, NG, SH).astype(jnp.float32)
        occ_cols = columns[..., :OG].reshape(block_vectors, NORB, OCC)
        extra = jnp.einsum("qpi,ia->qpa", occ_cols, amp_float).reshape(block_vectors, NORB, NG, VG)
        dressed = jnp.concatenate([columns[..., :OG], columns[..., OG:] + extra], axis=3)
        dressed = dressed.reshape(block_vectors, NORB, NORB).astype(jnp.bfloat16)
        dense = dressed.astype(jnp.float32)
        diagonal = jnp.diagonal(dense, axis1=1, axis2=2).reshape(block_vectors, NG, SH)[:, :, :OG]
        weight = jnp.sum(diagonal, axis=(1, 2))
        dcols = dense.reshape(block_vectors, NORB, NG, SH)[..., :OG].reshape(block_vectors, NORB, OCC)
        drows = dense.reshape(block_vectors, NG, SH, NORB)[:, :, :OG, :].reshape(block_vectors, OCC, NORB)
        coulomb = jnp.einsum("q,qab->ab", weight, dense)
        swapped = jnp.einsum("qpi,qib->pb", dcols, drows)
        return total + 2.0 * coulomb - swapped, dressed

    stacked = chol.reshape(Q // block_vectors, block_vectors, NORB, NORB)
    fock, dressed = lax.scan(one_block, jnp.zeros((NORB, NORB), jnp.float32), stacked)
    return dressed.reshape(Q, NORB, NORB), fock
```

```python
import jax
import jax.numpy as jnp
from jax import lax
from jax.sharding import Mesh
from jax.sharding import PartitionSpec as P

OG = 9
SH = 84
ROW = ("row_0", "row_1")
ALL = ("row_0", "row_1", "col_0", "col_1")


def gathered_copies(array, axis):
    copies = jnp.broadcast_to(array, (lax.axis_size(axis), *array.shape))
    return lax.all_to_all(copies, axis, split_axis=0, concat_axis=0, tiled=True)


def local(chol, amplitudes):
    q_local, row_width, col_width = chol.shape
    rows, cols = lax.axis_size(ROW), lax.axis_size(("col_0", "col_1"))
    q_own = q_local // (rows * cols)
    norb = rows * row_width
    groups = norb // SH
    pieces = lax.all_to_all(chol[:, None], ALL, split_axis=0, concat_axis=1, tiled=True)
    amp = gathered_copies(amplitudes, ROW)
    amp = jnp.transpose(amp, (1, 0, 2)).reshape(groups, OG, groups, SH - OG)
    amp = jnp.pad(amp, ((0, 0), (0, SH - OG), (0, 0), (OG, 0))).reshape(norb, norb)
    eye = jnp.eye(norb, dtype=jnp.bfloat16)
    pieces = pieces.reshape(q_own, rows, cols, row_width, col_width)
    whole = jnp.transpose(pieces, (0, 1, 3, 2, 4)).reshape(q_own, norb, norb)
    primed = jnp.einsum("pr,qrs->qps", eye - amp, whole, preferred_element_type=jnp.float32)
    primed = primed.astype(jnp.bfloat16)
    dressed = jnp.einsum("qpr,rs->qps", primed, eye + amp, preferred_element_type=jnp.float32)
    dressed = dressed.astype(jnp.bfloat16)
    occupied = jnp.arange(norb) % SH < OG
    diagonal = jnp.diagonal(dressed, axis1=1, axis2=2).astype(jnp.float32)
    weight = jnp.sum(jnp.where(occupied, diagonal, 0.0), axis=1)
    occ_cols = jnp.where(occupied, dressed, jnp.zeros_like(dressed))
    swapped = jnp.einsum("qpi,qir->pr", occ_cols, dressed, preferred_element_type=jnp.float32)
    fock = 2.0 * jnp.einsum("q,qpr->pr", weight, dressed.astype(jnp.float32)) - swapped
    fock = fock.astype(jnp.bfloat16).reshape(rows, row_width, cols // 2, 2, col_width)
    fock = jnp.transpose(fock, (3, 0, 2, 1, 4))
    fock = lax.all_to_all(fock, "col_1", split_axis=0, concat_axis=0, tiled=True)
    fock = jnp.sum(fock.astype(jnp.float32), axis=0).astype(jnp.bfloat16)
    fock = fock.reshape(rows * cols // 2, row_width, col_width)
    fock = lax.all_to_all(fock, (*ROW, "col_0"), split_axis=0, concat_axis=0, tiled=True)
    fock = jnp.sum(fock.astype(jnp.float32), axis=0).astype(jnp.bfloat16)
    other = lax.ppermute(fock, "pb", ((0, 1), (1, 0)))
    return dressed, fock.astype(jnp.float32) + other.astype(jnp.float32)


def solution(mesh):
    finer = Mesh(
        mesh.devices.reshape(mesh.shape["pb"], 4, 4, mesh.shape["col"] // 2, 2),
        ("pb", *ALL),
    )
    placed = (P("pb", ROW, ("col_0", "col_1")), P(None, ROW))
    return jax.shard_map(
        local,
        mesh=finer,
        in_specs=placed,
        out_specs=(P(("pb", *ALL), None, None), P(ROW, ("col_0", "col_1"))),
        check_vma=False,
    )
```

```python
import functools
import jax
import jax.numpy as jnp
from jax import lax
from jax.experimental import pallas as pl
from jax.experimental.pallas import tpu as pltpu
from jax.sharding import Mesh
from jax.sharding import PartitionSpec as P

OG, SH = 9, 84
RP, CP, WIN = 96, 384, 16


def dress(own, last, pieces, win, cols, sel, *rest):
    if last:
        before, unused, whole, fock, x, occ, stage, sem = rest
    else:
        whole, fock, x, occ, stage, sem = rest
    rows = x.shape[0] // RP
    blocks = x.shape[1] // CP
    width = pieces.shape[-1]
    per = rows // blocks
    x[...] = jnp.zeros_like(x)

    def place(r, carry):
        for c in range(blocks):
            x[pl.ds(pl.multiple_of(r * RP, RP), SH), c * CP : c * CP + width] = pieces[r * blocks + c, 0]
        return carry

    lax.fori_loop(0, rows, place, 0)
    for c in range(blocks):
        lanes = slice(c * CP, (c + 1) * CP)
        shift = jnp.dot(win[...], x[:, lanes], preferred_element_type=jnp.float32)
        for r in range(rows):
            at = slice(r * RP, r * RP + WIN)
            fixed = x[at, lanes].astype(jnp.float32) - shift[r * WIN : (r + 1) * WIN]
            x[at, lanes] = fixed.astype(jnp.bfloat16)
    deep = per * RP
    tall = per * SH

    def columns(m, carry):
        at = pl.ds(pl.multiple_of(m * deep, deep), deep)
        old = x[at, :]
        g = jnp.dot(old, sel[...], preferred_element_type=jnp.float32).astype(jnp.bfloat16)
        occ[at, :] = g
        extra = jnp.dot(g, cols[...], preferred_element_type=jnp.float32)
        new = (old.astype(jnp.float32) + extra).astype(jnp.bfloat16)
        x[at, :] = new
        for r in range(per):
            for c in range(blocks):
                block = new[r * RP : r * RP + SH, c * CP : c * CP + width]
                stage[m, r * SH : (r + 1) * SH, c * width : (c + 1) * width] = block
        pltpu.make_async_copy(
            stage.at[m], whole.at[own, pl.ds(pl.multiple_of(m * tall, tall), tall)], sem.at[m]
        ).start()
        return carry

    lax.fori_loop(0, blocks, columns, 0)
    inner = jnp.concatenate([occ[r * RP : r * RP + WIN, :] for r in range(rows)], axis=0)
    here = lax.broadcasted_iota(jnp.int32, inner.shape, 0)
    there = lax.broadcasted_iota(jnp.int32, inner.shape, 1)
    weight = 2.0 * jnp.sum(jnp.where(here == there, inner.astype(jnp.float32), 0.0))
    occ_rows = jnp.concatenate([x[r * RP : r * RP + WIN, :] for r in range(rows)], axis=0)

    def total(m, carry):
        at = pl.ds(pl.multiple_of(m * deep, deep), deep)
        swapped = jnp.dot(occ[at, :], occ_rows, preferred_element_type=jnp.float32)
        part = weight * x[at, :].astype(jnp.float32) - swapped
        if last:
            part = (part + before[at, :]).astype(jnp.bfloat16)
            for r in range(per):
                for c in range(blocks):
                    block = part[r * RP : r * RP + SH, c * CP : c * CP + width]
                    fock[c % 2, (m * per + r) * (blocks // 2) + c // 2] = block
        else:
            fock[at, :] = part
        return carry

    lax.fori_loop(0, blocks, total, 0)
    for m in range(blocks):
        pltpu.make_async_copy(
            stage.at[m], whole.at[own, m * tall : (m + 1) * tall], sem.at[m]
        ).wait()


def dress_call(own, pieces, win, cols, sel, before=None, whole=None, q_own=2):
    last = before is not None
    rows = win.shape[0] // WIN
    blocks = pieces.shape[0] // rows
    norb = rows * SH
    width = pieces.shape[-1]
    vmem, hbm = pl.BlockSpec(memory_space=pltpu.VMEM), pl.BlockSpec(memory_space=pl.ANY)
    wide = rows * RP
    if last:
        fock = jax.ShapeDtypeStruct((2, rows * blocks // 2, SH, width), jnp.bfloat16)
    else:
        fock = jax.ShapeDtypeStruct((wide, blocks * CP), jnp.float32)
    args = (pieces, win, cols, sel) + ((before, whole) if last else ())
    return pl.pallas_call(
        functools.partial(dress, own, last),
        out_shape=(jax.ShapeDtypeStruct((q_own, norb, norb), jnp.bfloat16), fock),
        in_specs=[vmem] * 4 + ([vmem, hbm] if last else []),
        out_specs=(hbm, vmem),
        input_output_aliases={5: 0} if last else {},
        scratch_shapes=[
            pltpu.VMEM((wide, blocks * CP), jnp.bfloat16),
            pltpu.VMEM((wide, rows * WIN), jnp.bfloat16),
            pltpu.VMEM((blocks, rows // blocks * SH, norb), jnp.bfloat16),
            pltpu.SemaphoreType.DMA((blocks,)),
        ],
        compiler_params=pltpu.CompilerParams(vmem_limit_bytes=60 * 2**20),
        name="dress_last" if last else "dress_first",
    )(*args)


def tables(amp, blocks):
    groups = amp.shape[0]
    cut = amp.reshape(groups, groups, OG, SH - OG)
    cut = jnp.pad(cut, ((0, 0), (0, 0), (0, WIN - OG), (OG, 0))).reshape(groups, groups * WIN, SH)
    win = jnp.pad(cut, ((0, 0), (0, 0), (0, RP - SH)))
    win = jnp.transpose(win, (1, 0, 2)).reshape(groups * WIN, groups * RP)
    per = groups // blocks
    cols = jnp.transpose(cut, (1, 0, 2)).reshape(groups * WIN, blocks, per * SH)
    cols = jnp.pad(cols, ((0, 0), (0, 0), (0, CP - per * SH))).reshape(groups * WIN, blocks * CP)
    at = lax.broadcasted_iota(jnp.int32, (blocks * CP, groups * WIN), 0)
    to = lax.broadcasted_iota(jnp.int32, (blocks * CP, groups * WIN), 1)
    inside = at % CP
    group = at // CP * per + inside // SH
    hit = (inside < per * SH) & (to // WIN == group) & (to % WIN == inside % SH) & (inside % SH < OG)
    return win, cols, hit.astype(jnp.bfloat16)


ROW = ("row_0", "row_1")
COL = ("col_0", "col_1")
ALL = (*ROW, *COL)


def swap(array, axis):
    return lax.all_to_all(array, axis, split_axis=0, concat_axis=0, tiled=True)


def local(chol, amplitudes):
    q_local, row_width, col_width = chol.shape
    devices = lax.axis_size(ALL)
    cols = lax.axis_size(COL)
    q_own = q_local // devices
    sent = chol.reshape(devices, q_own, 1, row_width, col_width)
    first = swap(sent[:, 0], ALL)
    amp = swap(jnp.broadcast_to(amplitudes, (lax.axis_size(ROW), *amplitudes.shape)), ROW)
    win, into, sel = tables(amp, cols)
    second = swap(sent[:, 1], ALL)
    whole, part = dress_call(0, first, win, into, sel)
    whole, fock = dress_call(1, second, win, into, sel, part, whole)
    fock = swap(fock, "col_1")
    fock = (fock[0].astype(jnp.float32) + fock[1].astype(jnp.float32)).astype(jnp.bfloat16)
    fock = swap(fock, (*ROW, "col_0"))
    fock = jnp.sum(fock.astype(jnp.float32), axis=0).astype(jnp.bfloat16)
    other = lax.ppermute(fock, "pb", ((0, 1), (1, 0)))
    return whole, fock.astype(jnp.float32) + other.astype(jnp.float32)


def solution(mesh):
    finer = Mesh(
        mesh.devices.reshape(mesh.shape["pb"], 4, 4, mesh.shape["col"] // 2, 2),
        ("pb", *ALL),
    )
    placed = (P("pb", ROW, COL), P(None, ROW))
    return jax.shard_map(
        local,
        mesh=finer,
        in_specs=placed,
        out_specs=(P(("pb", *ALL), None, None), P(ROW, COL)),
        check_vma=False,
    )
```

```python
import functools

import jax
import jax.numpy as jnp
from jax import lax
from jax.experimental import pallas as pl
from jax.experimental.pallas import tpu as pltpu
from jax.sharding import Mesh
from jax.sharding import PartitionSpec as P

OG, SH = 9, 84
RP, CP, WIN = 96, 384, 16
FULL, LANES, TALL, LONG = 80, 256, 28, 112
VMEM = pl.BlockSpec(memory_space=pltpu.VMEM)
HBM = pl.BlockSpec(memory_space=pltpu.HBM)


def hot(condition):
    return jnp.where(condition, 1.0, 0.0).astype(jnp.bfloat16)


def pack(own, q_own, source, out, held, wire, sem, sent):
    height, width, depth = held.shape
    rest = width - LANES
    devices = depth // q_own
    spans = [(at, min(WIN, height - at)) for at in range(0, height, WIN)]
    copies = [
        pltpu.make_async_copy(source.at[at : at + n], held.at[at : at + n], sem.at[k])
        for k, (at, n) in enumerate(spans)
    ]
    for copy in copies:
        copy.start()
    row = lax.broadcasted_iota(jnp.int32, (devices, depth), 0)
    col = lax.broadcasted_iota(jnp.int32, (devices, depth), 1)
    pick = hot(col == row * q_own + own)
    row = lax.broadcasted_iota(jnp.int32, (LANES, LANES), 0)
    col = lax.broadcasted_iota(jnp.int32, (LANES, LANES), 1)
    turn = hot((row // WIN == col % WIN) & (row % WIN == col // WIN))
    zeros = jnp.zeros((LANES - 3 * rest, depth), jnp.bfloat16)

    def slab(k):
        if k < FULL:
            return held[k, :LANES, :]
        k -= FULL
        if k >= TALL:
            return held[FULL + k - TALL, :LANES, :]
        parts = [held[i * TALL + k, LANES:, :] for i in range(3)]
        return jnp.concatenate(parts + [zeros], axis=0)

    for g in range(LONG // WIN):
        if g < FULL // WIN:
            copies[g].wait()
        elif g == FULL // WIN:
            for copy in copies[g:]:
                copy.wait()
        flat = [
            lax.dot_general(
                pick, slab(g * WIN + k), (((1,), (1,)), ((), ())), preferred_element_type=jnp.float32
            ).astype(jnp.bfloat16)
            for k in range(WIN)
        ]
        for t in range(devices // WIN):
            mixed = jnp.concatenate([f[t * WIN : (t + 1) * WIN] for f in flat], axis=0)
            done = jnp.dot(turn, mixed, preferred_element_type=jnp.float32).astype(jnp.bfloat16)
            done = done.reshape(WIN, WIN, LANES)
            wire[g, t * WIN : (t + 1) * WIN] = done
        pltpu.make_async_copy(wire.at[g], out.at[:, g * WIN : (g + 1) * WIN], sent.at[g]).start()
    for g in range(LONG // WIN):
        pltpu.make_async_copy(wire.at[g], out.at[:, g * WIN : (g + 1) * WIN], sent.at[g]).wait()


def pack_call(own, q_own, source):
    height, _, depth = source.shape
    source = pltpu.with_memory_space_constraint(source, pltpu.HBM)
    return pl.pallas_call(
        functools.partial(pack, own, q_own),
        out_shape=pltpu.HBM((depth // q_own, LONG, LANES), jnp.bfloat16),
        in_specs=[HBM],
        out_specs=HBM,
        scratch_shapes=[
            pltpu.VMEM(source.shape, jnp.bfloat16),
            pltpu.VMEM((LONG // WIN, depth // q_own, WIN, LANES), jnp.bfloat16),
            pltpu.SemaphoreType.DMA((-(-height // WIN),)),
            pltpu.SemaphoreType.DMA((LONG // WIN,)),
        ],
        compiler_params=pltpu.CompilerParams(vmem_limit_bytes=20 * 2**20),
        cost_estimate=pl.CostEstimate(flops=5 * 10**9, bytes_accessed=10**7, transcendentals=0),
        name="pack",
    )(source)


def dress(own, last, pieces, win, cols, sel, *rest):
    if last:
        core, before, _, whole, mine, theirs, held, x, top, stage, hsem, sem, fock, fsem = rest
    else:
        whole, kept, held, x, top, stage, hsem, sem, fock, fsem = rest
    rows = x.shape[0]
    blocks = x.shape[2] // CP
    width = stage.shape[1] // blocks
    side = width - LANES
    per = rows // blocks
    deep, tall = per * RP, per * SH

    def come(m):
        part = pl.ds(m * per * blocks, per * blocks)
        return pltpu.make_async_copy(pieces.at[part], held.at[part], hsem.at[m])

    def leave(m):
        part = pl.ds(m * tall, tall)
        return pltpu.make_async_copy(stage.at[part], whole.at[own, part], sem.at[m])

    def carried(m):
        if last:
            return pltpu.make_async_copy(before.at[m], fock.at[m], fsem.at[m])
        return pltpu.make_async_copy(fock.at[m], kept.at[m], fsem.at[m])

    for m in range(blocks):
        come(m).start()
    if last:
        for m in range(blocks):
            carried(m).start()
    for c in range(blocks):
        x[:, :, c * CP + width : (c + 1) * CP] = jnp.zeros((rows, RP, CP - width), jnp.bfloat16)
    x[:, FULL:, :] = jnp.zeros((rows, RP - FULL, blocks * CP), jnp.bfloat16)

    def place(r, carry):
        for c in range(blocks):
            at = r * blocks + c
            lane = c * CP
            x[r, :FULL, lane : lane + LANES] = held[at, :FULL, :]
            x[r, FULL:SH, lane : lane + LANES] = held[at, FULL + TALL :, :]
            for i in range(3):
                x[r, i * TALL : (i + 1) * TALL, lane + LANES : lane + width] = held[
                    at, FULL : FULL + TALL, i * side : (i + 1) * side
                ]
        return carry

    for m in range(blocks):
        come(m).wait()
        lax.fori_loop(m * per, (m + 1) * per, place, 0)
    flat = x.reshape(rows * RP, blocks * CP)
    shift = jnp.dot(win[...], flat[...], preferred_element_type=jnp.float32)
    for r in range(rows):
        at = slice(r * RP, r * RP + WIN)
        fixed = flat[at, :].astype(jnp.float32) - shift[r * WIN : (r + 1) * WIN]
        flat[at, :] = fixed.astype(jnp.bfloat16)
    g = jnp.dot(flat[...], sel[...], preferred_element_type=jnp.float32).astype(jnp.bfloat16)
    inner = jnp.concatenate([g[r * RP : r * RP + WIN, :] for r in range(rows)], axis=0)
    here = lax.broadcasted_iota(jnp.int32, inner.shape, 0)
    there = lax.broadcasted_iota(jnp.int32, inner.shape, 1)
    weight = 2.0 * jnp.sum(jnp.where(here == there, inner.astype(jnp.float32), 0.0))
    for m in range(blocks):
        at = slice(m * deep, (m + 1) * deep)
        extra = jnp.dot(g[at], cols[...], preferred_element_type=jnp.float32)
        new = (flat[at, :].astype(jnp.float32) + extra).astype(jnp.bfloat16)
        flat[at, :] = new
        for r in range(per):
            for c in range(blocks):
                block = new[r * RP : r * RP + SH, c * CP : c * CP + width]
                down = m * tall + r * SH
                stage[down : down + SH, c * width : (c + 1) * width] = block
            to = (m * per + r) * WIN
            top[to : to + WIN, :] = new[r * RP : r * RP + WIN, :]
        leave(m).start()

    def wired(target, at, block):
        target[at, :FULL, :] = block[:FULL, :LANES]
        target[at, FULL + TALL :, :] = block[FULL:, :LANES]
        for i in range(3):
            target[at, FULL : FULL + TALL, i * side : (i + 1) * side] = block[
                i * TALL : (i + 1) * TALL, LANES:
            ]
        target[at, FULL : FULL + TALL, 3 * side :] = jnp.zeros(
            (TALL, LANES - 3 * side), jnp.bfloat16
        )

    for m in range(blocks):
        at = slice(m * deep, (m + 1) * deep)
        swapped = jnp.dot(g[at], top[...], preferred_element_type=jnp.float32)
        total = weight * flat[at, :].astype(jnp.float32) - swapped
        if not last:
            fock[m] = total
            carried(m).start()
            continue
        odd = core[0] == 1
        carried(m).wait()
        total = (total + fock[m]).astype(jnp.bfloat16)
        for r in range(per):
            for h in range(blocks // 2):
                pair = [
                    total[r * RP : r * RP + SH, c * CP : c * CP + width] for c in (2 * h, 2 * h + 1)
                ]
                to = (m * per + r) * (blocks // 2) + h
                wired(mine, to, jnp.where(odd, pair[1], pair[0]))
                wired(theirs, to, jnp.where(odd, pair[0], pair[1]))
    for m in range(blocks):
        leave(m).wait()
        if not last:
            carried(m).wait()


def dress_call(own, q_own, shape, pieces, win, cols, sel, core=None, before=None, whole=None):
    last = before is not None
    rows, blocks, _ = shape
    norb = rows * SH
    pieces = pltpu.with_memory_space_constraint(pieces, pltpu.HBM)
    half = pltpu.VMEM((rows * blocks // 2, LONG, LANES), jnp.bfloat16)
    split = (blocks, rows // blocks * RP, blocks * CP)
    whole_shape = pltpu.HBM((q_own, norb, norb), jnp.bfloat16)
    if last:
        before = pltpu.with_memory_space_constraint(before, pltpu.HBM)
        args = (pieces, win, cols, sel, core, before, whole)
        in_specs = [HBM, VMEM, VMEM, VMEM, pl.BlockSpec(memory_space=pltpu.SMEM), HBM, HBM]
        out_shape, out_specs = (whole_shape, half, half), (HBM, VMEM, VMEM)
    else:
        args = (pieces, win, cols, sel)
        in_specs = [HBM, VMEM, VMEM, VMEM]
        out_shape = (whole_shape, pltpu.HBM(split, jnp.float32))
        out_specs = (HBM, HBM)
    sem = pltpu.SemaphoreType.DMA((blocks,))
    return pl.pallas_call(
        functools.partial(dress, own, last),
        out_shape=out_shape,
        in_specs=in_specs,
        out_specs=out_specs,
        input_output_aliases={6: 0} if last else {},
        scratch_shapes=[
            pltpu.VMEM(pieces.shape, jnp.bfloat16),
            pltpu.VMEM((rows, RP, blocks * CP), jnp.bfloat16),
            pltpu.VMEM((rows * WIN, blocks * CP), jnp.bfloat16),
            pltpu.VMEM((norb, norb), jnp.bfloat16),
            sem,
            sem,
            pltpu.VMEM(split, jnp.float32),
            sem,
        ],
        compiler_params=pltpu.CompilerParams(vmem_limit_bytes=48 * 2**20),
        cost_estimate=pl.CostEstimate(flops=10**10, bytes_accessed=10**7, transcendentals=0),
        name="dress_last" if last else "dress_first",
    )(*args)


def finish(own, other, fock):
    width = fock.shape[1]
    side = width - LANES
    total = own[...].astype(jnp.float32) + other[...].astype(jnp.float32)
    fock[:FULL, :LANES] = total[:FULL]
    fock[FULL:, :LANES] = total[FULL + TALL :]
    for i in range(3):
        fock[i * TALL : (i + 1) * TALL, LANES:] = total[
            FULL : FULL + TALL, i * side : (i + 1) * side
        ]


def finish_call(own, other, width):
    return pl.pallas_call(
        finish,
        out_shape=jax.ShapeDtypeStruct((SH, width), jnp.float32),
        in_specs=[VMEM] * 2,
        out_specs=VMEM,
        name="finish",
    )(own, other)


def tables(amp, blocks):
    groups = amp.shape[0]
    cut = amp.reshape(groups, groups, OG, SH - OG)
    cut = jnp.pad(cut, ((0, 0), (0, 0), (0, WIN - OG), (OG, 0))).reshape(groups, groups * WIN, SH)
    win = jnp.pad(cut, ((0, 0), (0, 0), (0, RP - SH)))
    win = jnp.transpose(win, (1, 0, 2)).reshape(groups * WIN, groups * RP)
    per = groups // blocks
    cols = jnp.transpose(cut, (1, 0, 2)).reshape(groups * WIN, blocks, per * SH)
    cols = jnp.pad(cols, ((0, 0), (0, 0), (0, CP - per * SH))).reshape(groups * WIN, blocks * CP)
    at = lax.broadcasted_iota(jnp.int32, (blocks * CP, groups * WIN), 0)
    to = lax.broadcasted_iota(jnp.int32, (blocks * CP, groups * WIN), 1)
    inside = at % CP
    group = at // CP * per + inside // SH
    hit = (inside < per * SH) & (to // WIN == group) & (to % WIN == inside % SH) & (inside % SH < OG)
    return win, cols, hit.astype(jnp.bfloat16)


ROW = ("row_0", "row_1")
COL = ("col_0", "col_1")
ALL = (*ROW, *COL)


def swap(array, axis):
    return lax.all_to_all(array, axis, split_axis=0, concat_axis=0, tiled=True)


def all_of(array, axis):
    count = lax.axis_size(axis)
    here = lax.axis_index(axis)
    found = [array]
    for step in range(1, count):
        pairs = [((to + step) % count, to) for to in range(count)]
        found.append(lax.ppermute(array, axis, pairs))
    found = jnp.stack(found + found[:-1])
    return lax.dynamic_slice_in_dim(found, (count - here) % count, count, 0)


def step(chol, amplitudes):
    q_local, _, col_width = chol.shape
    shape = (lax.axis_size(ROW), lax.axis_size(COL), col_width)
    q_own = q_local // lax.axis_size(ALL)
    source = jnp.transpose(chol, (1, 2, 0))
    sent, amplitudes = lax.optimization_barrier((pack_call(0, q_own, source), amplitudes))
    first = swap(sent, ALL)
    amp = all_of(amplitudes, ROW)
    win, into, sel = tables(amp, shape[1])
    second = swap(pack_call(1, q_own, source), ALL)
    core = lax.axis_index("col_1").astype(jnp.int32).reshape(1)
    whole, part = dress_call(0, q_own, shape, first, win, into, sel)
    whole, mine, theirs = dress_call(1, q_own, shape, second, win, into, sel, core, part, whole)
    came = lax.ppermute(theirs, "col_1", ((0, 1), (1, 0)))
    fock = (mine.astype(jnp.float32) + came.astype(jnp.float32)).astype(jnp.bfloat16)
    fock = swap(fock, (*ROW, "col_0"))
    fock = jnp.sum(fock.astype(jnp.float32), axis=0).astype(jnp.bfloat16)
    other = lax.ppermute(fock, "pb", ((0, 1), (1, 0)))
    return whole, finish_call(fock, other, col_width)


def solution(mesh):
    finer = Mesh(
        mesh.devices.reshape(mesh.shape["pb"], 4, 4, mesh.shape["col"] // 2, 2),
        ("pb", *ALL),
    )
    placed = (P("pb", ROW, COL), P(None, ROW))
    return jax.shard_map(
        step,
        mesh=finer,
        in_specs=placed,
        out_specs=(P(("pb", *ALL), None, None), P(ROW, COL)),
        check_vma=False,
    )
```

```python
import functools

import jax
import jax.numpy as jnp
from jax import lax
from jax.experimental import pallas as pl
from jax.experimental.pallas import tpu as pltpu
from jax.sharding import Mesh
from jax.sharding import PartitionSpec as P

OG, SH = 9, 84
RP, CP, WIN = 96, 384, 16
FULL, LANES, TALL, LONG = 80, 256, 28, 112
VMEM = pl.BlockSpec(memory_space=pltpu.VMEM)
HBM = pl.BlockSpec(memory_space=pltpu.HBM)


def hot(condition):
    return jnp.where(condition, 1.0, 0.0).astype(jnp.bfloat16)


def pack(own, q_own, source, out, held, wire, sem, sent):
    height, width, depth = held.shape
    rest = width - LANES
    devices = depth // q_own
    spans = [(at, min(WIN, height - at)) for at in range(0, height, WIN)]
    copies = [
        pltpu.make_async_copy(source.at[at : at + n], held.at[at : at + n], sem.at[k])
        for k, (at, n) in enumerate(spans)
    ]
    for copy in copies:
        copy.start()
    row = lax.broadcasted_iota(jnp.int32, (devices, depth), 0)
    col = lax.broadcasted_iota(jnp.int32, (devices, depth), 1)
    pick = hot(col == row * q_own + own)
    row = lax.broadcasted_iota(jnp.int32, (LANES, LANES), 0)
    col = lax.broadcasted_iota(jnp.int32, (LANES, LANES), 1)
    turn = hot((row // WIN == col % WIN) & (row % WIN == col // WIN))
    zeros = jnp.zeros((LANES - 3 * rest, depth), jnp.bfloat16)

    def slab(k):
        if k < FULL:
            return held[k, :LANES, :]
        k -= FULL
        if k >= TALL:
            return held[FULL + k - TALL, :LANES, :]
        parts = [held[i * TALL + k, LANES:, :] for i in range(3)]
        return jnp.concatenate(parts + [zeros], axis=0)

    for g in range(LONG // WIN):
        if g < FULL // WIN:
            copies[g].wait()
        elif g == FULL // WIN:
            for copy in copies[g:]:
                copy.wait()
        flat = [
            lax.dot_general(
                pick, slab(g * WIN + k), (((1,), (1,)), ((), ())), preferred_element_type=jnp.float32
            ).astype(jnp.bfloat16)
            for k in range(WIN)
        ]
        for t in range(devices // WIN):
            mixed = jnp.concatenate([f[t * WIN : (t + 1) * WIN] for f in flat], axis=0)
            done = jnp.dot(turn, mixed, preferred_element_type=jnp.float32).astype(jnp.bfloat16)
            done = done.reshape(WIN, WIN, LANES)
            wire[g, t * WIN : (t + 1) * WIN] = done
        pltpu.make_async_copy(wire.at[g], out.at[:, g * WIN : (g + 1) * WIN], sent.at[g]).start()
    for g in range(LONG // WIN):
        pltpu.make_async_copy(wire.at[g], out.at[:, g * WIN : (g + 1) * WIN], sent.at[g]).wait()


def pack_call(own, q_own, source):
    height, _, depth = source.shape
    source = pltpu.with_memory_space_constraint(source, pltpu.HBM)
    return pl.pallas_call(
        functools.partial(pack, own, q_own),
        out_shape=pltpu.HBM((depth // q_own, LONG, LANES), jnp.bfloat16),
        in_specs=[HBM],
        out_specs=HBM,
        scratch_shapes=[
            pltpu.VMEM(source.shape, jnp.bfloat16),
            pltpu.VMEM((LONG // WIN, depth // q_own, WIN, LANES), jnp.bfloat16),
            pltpu.SemaphoreType.DMA((-(-height // WIN),)),
            pltpu.SemaphoreType.DMA((LONG // WIN,)),
        ],
        compiler_params=pltpu.CompilerParams(vmem_limit_bytes=20 * 2**20),
        cost_estimate=pl.CostEstimate(flops=5 * 10**9, bytes_accessed=10**7, transcendentals=0),
        name="pack",
    )(source)


def dress(own, last, pieces, win, cols, sel, *rest):
    if last:
        core, before, _, whole, mine, theirs, held, x, top, stage, hsem, sem, fock, fsem = rest
    else:
        whole, kept, held, x, top, stage, hsem, sem, fock, fsem = rest
    rows = x.shape[0]
    blocks = x.shape[2] // CP
    width = stage.shape[1] // blocks
    side = width - LANES
    per = rows // blocks
    deep, tall = per * RP, per * SH

    def come(m):
        part = pl.ds(m * per * blocks, per * blocks)
        return pltpu.make_async_copy(pieces.at[part], held.at[part], hsem.at[m])

    def leave(m):
        part = pl.ds(m * tall, tall)
        return pltpu.make_async_copy(stage.at[part], whole.at[own, part], sem.at[m])

    def carried(m):
        if last:
            return pltpu.make_async_copy(before.at[m], fock.at[m], fsem.at[m])
        return pltpu.make_async_copy(fock.at[m], kept.at[m], fsem.at[m])

    for m in range(blocks):
        come(m).start()
    if last:
        for m in range(blocks):
            carried(m).start()
    for c in range(blocks):
        x[:, :, c * CP + width : (c + 1) * CP] = jnp.zeros((rows, RP, CP - width), jnp.bfloat16)
    x[:, FULL:, :] = jnp.zeros((rows, RP - FULL, blocks * CP), jnp.bfloat16)

    def place(r, carry):
        for c in range(blocks):
            at = r * blocks + c
            lane = c * CP
            x[r, :FULL, lane : lane + LANES] = held[at, :FULL, :]
            x[r, FULL:SH, lane : lane + LANES] = held[at, FULL + TALL :, :]
            for i in range(3):
                x[r, i * TALL : (i + 1) * TALL, lane + LANES : lane + width] = held[
                    at, FULL : FULL + TALL, i * side : (i + 1) * side
                ]
        return carry

    for m in range(blocks):
        come(m).wait()
        lax.fori_loop(m * per, (m + 1) * per, place, 0)
    flat = x.reshape(rows * RP, blocks * CP)
    shift = jnp.dot(win[...], flat[...], preferred_element_type=jnp.float32)
    for r in range(rows):
        at = slice(r * RP, r * RP + WIN)
        fixed = flat[at, :].astype(jnp.float32) - shift[r * WIN : (r + 1) * WIN]
        flat[at, :] = fixed.astype(jnp.bfloat16)
    g = jnp.dot(flat[...], sel[...], preferred_element_type=jnp.float32).astype(jnp.bfloat16)
    inner = jnp.concatenate([g[r * RP : r * RP + WIN, :] for r in range(rows)], axis=0)
    here = lax.broadcasted_iota(jnp.int32, inner.shape, 0)
    there = lax.broadcasted_iota(jnp.int32, inner.shape, 1)
    weight = 2.0 * jnp.sum(jnp.where(here == there, inner.astype(jnp.float32), 0.0))
    for m in range(blocks):
        at = slice(m * deep, (m + 1) * deep)
        extra = jnp.dot(g[at], cols[...], preferred_element_type=jnp.float32)
        new = (flat[at, :].astype(jnp.float32) + extra).astype(jnp.bfloat16)
        flat[at, :] = new
        for r in range(per):
            for c in range(blocks):
                block = new[r * RP : r * RP + SH, c * CP : c * CP + width]
                down = m * tall + r * SH
                stage[down : down + SH, c * width : (c + 1) * width] = block
            to = (m * per + r) * WIN
            top[to : to + WIN, :] = new[r * RP : r * RP + WIN, :]
        leave(m).start()

    def wired(target, at, block):
        target[at, :FULL, :] = block[:FULL, :LANES]
        target[at, FULL + TALL :, :] = block[FULL:, :LANES]
        for i in range(3):
            target[at, FULL : FULL + TALL, i * side : (i + 1) * side] = block[
                i * TALL : (i + 1) * TALL, LANES:
            ]
        target[at, FULL : FULL + TALL, 3 * side :] = jnp.zeros(
            (TALL, LANES - 3 * side), jnp.bfloat16
        )

    for m in range(blocks):
        at = slice(m * deep, (m + 1) * deep)
        swapped = jnp.dot(g[at], top[...], preferred_element_type=jnp.float32)
        total = weight * flat[at, :].astype(jnp.float32) - swapped
        if not last:
            fock[m] = total.astype(jnp.bfloat16)
            carried(m).start()
            continue
        odd = core[0] == 1
        carried(m).wait()
        total = (total + fock[m].astype(jnp.float32)).astype(jnp.bfloat16)
        for r in range(per):
            for h in range(blocks // 2):
                pair = [
                    total[r * RP : r * RP + SH, c * CP : c * CP + width] for c in (2 * h, 2 * h + 1)
                ]
                to = (m * per + r) * (blocks // 2) + h
                wired(mine, to, jnp.where(odd, pair[1], pair[0]))
                wired(theirs, to, jnp.where(odd, pair[0], pair[1]))
    for m in range(blocks):
        leave(m).wait()
        if not last:
            carried(m).wait()


def dress_call(own, q_own, shape, pieces, win, cols, sel, core=None, before=None, whole=None):
    last = before is not None
    rows, blocks, _ = shape
    norb = rows * SH
    pieces = pltpu.with_memory_space_constraint(pieces, pltpu.HBM)
    half = pltpu.VMEM((rows * blocks // 2, LONG, LANES), jnp.bfloat16)
    split = (blocks, rows // blocks * RP, blocks * CP)
    whole_shape = pltpu.HBM((q_own, norb, norb), jnp.bfloat16)
    if last:
        before = pltpu.with_memory_space_constraint(before, pltpu.HBM)
        args = (pieces, win, cols, sel, core, before, whole)
        in_specs = [HBM, VMEM, VMEM, VMEM, pl.BlockSpec(memory_space=pltpu.SMEM), HBM, HBM]
        out_shape, out_specs = (whole_shape, half, half), (HBM, VMEM, VMEM)
    else:
        args = (pieces, win, cols, sel)
        in_specs = [HBM, VMEM, VMEM, VMEM]
        out_shape = (whole_shape, pltpu.HBM(split, jnp.bfloat16))
        out_specs = (HBM, HBM)
    sem = pltpu.SemaphoreType.DMA((blocks,))
    return pl.pallas_call(
        functools.partial(dress, own, last),
        out_shape=out_shape,
        in_specs=in_specs,
        out_specs=out_specs,
        input_output_aliases={6: 0} if last else {},
        scratch_shapes=[
            pltpu.VMEM(pieces.shape, jnp.bfloat16),
            pltpu.VMEM((rows, RP, blocks * CP), jnp.bfloat16),
            pltpu.VMEM((rows * WIN, blocks * CP), jnp.bfloat16),
            pltpu.VMEM((norb, norb), jnp.bfloat16),
            sem,
            sem,
            pltpu.VMEM(split, jnp.bfloat16),
            sem,
        ],
        compiler_params=pltpu.CompilerParams(vmem_limit_bytes=48 * 2**20),
        cost_estimate=pl.CostEstimate(flops=10**10, bytes_accessed=10**7, transcendentals=0),
        name="dress_last" if last else "dress_first",
    )(*args)


def finish(own, other, fock):
    width = fock.shape[1]
    side = width - LANES
    total = own[...].astype(jnp.float32) + other[...].astype(jnp.float32)
    fock[:FULL, :LANES] = total[:FULL]
    fock[FULL:, :LANES] = total[FULL + TALL :]
    for i in range(3):
        fock[i * TALL : (i + 1) * TALL, LANES:] = total[
            FULL : FULL + TALL, i * side : (i + 1) * side
        ]


def finish_call(own, other, width):
    own = pltpu.with_memory_space_constraint(own, pltpu.VMEM)
    other = pltpu.with_memory_space_constraint(other, pltpu.VMEM)
    return pl.pallas_call(
        finish,
        out_shape=jax.ShapeDtypeStruct((SH, width), jnp.float32),
        in_specs=[VMEM] * 2,
        out_specs=VMEM,
        name="finish",
    )(own, other)


def join(here, *refs):
    count = len(refs) - 1
    for step in range(count):
        refs[-1][lax.rem(here[0] + step, count)] = refs[step][...]


def join_call(here, parts):
    return pl.pallas_call(
        join,
        out_shape=jax.ShapeDtypeStruct((len(parts), *parts[0].shape), parts[0].dtype),
        in_specs=[pl.BlockSpec(memory_space=pltpu.SMEM)] + [VMEM] * len(parts),
        out_specs=VMEM,
        name="join",
    )(here, *parts)


def tables(amp, blocks):
    groups = amp.shape[0]
    cut = amp.reshape(groups, groups, OG, SH - OG)
    cut = jnp.pad(cut, ((0, 0), (0, 0), (0, WIN - OG), (OG, 0))).reshape(groups, groups * WIN, SH)
    win = jnp.pad(cut, ((0, 0), (0, 0), (0, RP - SH)))
    win = jnp.transpose(win, (1, 0, 2)).reshape(groups * WIN, groups * RP)
    per = groups // blocks
    cols = jnp.transpose(cut, (1, 0, 2)).reshape(groups * WIN, blocks, per * SH)
    cols = jnp.pad(cols, ((0, 0), (0, 0), (0, CP - per * SH))).reshape(groups * WIN, blocks * CP)
    at = lax.broadcasted_iota(jnp.int32, (blocks * CP, groups * WIN), 0)
    to = lax.broadcasted_iota(jnp.int32, (blocks * CP, groups * WIN), 1)
    inside = at % CP
    group = at // CP * per + inside // SH
    hit = (inside < per * SH) & (to // WIN == group) & (to % WIN == inside % SH) & (inside % SH < OG)
    return win, cols, hit.astype(jnp.bfloat16)


ROW = ("row_0", "row_1")
COL = ("col_0", "col_1")
ALL = (*ROW, *COL)


def swap(array, axis):
    return lax.all_to_all(array, axis, split_axis=0, concat_axis=0, tiled=True)


def all_of(array, axis):
    count = lax.axis_size(axis)
    here = lax.axis_index(axis)
    found = [array]
    for step in range(1, count):
        pairs = [((to + step) % count, to) for to in range(count)]
        found.append(lax.ppermute(array, axis, pairs))
    return join_call(here.astype(jnp.int32).reshape(1), found)


def step(chol, amplitudes):
    q_local, _, col_width = chol.shape
    shape = (lax.axis_size(ROW), lax.axis_size(COL), col_width)
    q_own = q_local // lax.axis_size(ALL)
    source = jnp.transpose(chol, (1, 2, 0))
    sent, amplitudes = lax.optimization_barrier((pack_call(0, q_own, source), amplitudes))
    first = swap(sent, ALL)
    amp = all_of(amplitudes, ROW)
    win, into, sel = tables(amp, shape[1])
    second = swap(pack_call(1, q_own, source), ALL)
    core = lax.axis_index("col_1").astype(jnp.int32).reshape(1)
    whole, part = dress_call(0, q_own, shape, first, win, into, sel)
    whole, mine, theirs = dress_call(1, q_own, shape, second, win, into, sel, core, part, whole)
    came = lax.ppermute(theirs, "col_1", ((0, 1), (1, 0)))
    fock = (mine.astype(jnp.float32) + came.astype(jnp.float32)).astype(jnp.bfloat16)
    fock = swap(fock, (*ROW, "col_0"))
    fock = jnp.sum(fock.astype(jnp.float32), axis=0).astype(jnp.bfloat16)
    other = lax.ppermute(fock, "pb", ((0, 1), (1, 0)))
    return whole, finish_call(fock, other, col_width)


def solution(mesh):
    finer = Mesh(
        mesh.devices.reshape(mesh.shape["pb"], 4, 4, mesh.shape["col"] // 2, 2),
        ("pb", *ALL),
    )
    placed = (P("pb", ROW, COL), P(None, ROW))
    return jax.shard_map(
        step,
        mesh=finer,
        in_specs=placed,
        out_specs=(P(("pb", *ALL), None, None), P(ROW, COL)),
        check_vma=False,
    )
```

```python
import functools

import jax
import jax.numpy as jnp
from jax import lax
from jax.experimental import pallas as pl
from jax.experimental.pallas import tpu as pltpu
from jax.sharding import Mesh
from jax.sharding import PartitionSpec as P

OG, SH = 9, 84
RP, CP, WIN = 96, 384, 16
FULL, LANES, TALL, LONG = 80, 256, 28, 112
VMEM = pl.BlockSpec(memory_space=pltpu.VMEM)
HBM = pl.BlockSpec(memory_space=pltpu.HBM)


def hot(condition):
    return jnp.where(condition, 1.0, 0.0).astype(jnp.bfloat16)


def pack(own, q_own, source, out, held, wire, sem, sent):
    height, width, depth = held.shape
    rest = width - LANES
    devices = depth // q_own
    spans = [(at, min(WIN, height - at)) for at in range(0, height, WIN)]
    copies = [
        pltpu.make_async_copy(source.at[at : at + n], held.at[at : at + n], sem.at[k])
        for k, (at, n) in enumerate(spans)
    ]
    for copy in copies:
        copy.start()
    row = lax.broadcasted_iota(jnp.int32, (devices, depth), 0)
    col = lax.broadcasted_iota(jnp.int32, (devices, depth), 1)
    pick = hot(col == row * q_own + own)
    row = lax.broadcasted_iota(jnp.int32, (LANES, LANES), 0)
    col = lax.broadcasted_iota(jnp.int32, (LANES, LANES), 1)
    turn = hot((row // WIN == col % WIN) & (row % WIN == col // WIN))
    zeros = jnp.zeros((LANES - 3 * rest, depth), jnp.bfloat16)

    def slab(k):
        if k < FULL:
            return held[k, :LANES, :]
        k -= FULL
        if k >= TALL:
            return held[FULL + k - TALL, :LANES, :]
        parts = [held[i * TALL + k, LANES:, :] for i in range(3)]
        return jnp.concatenate(parts + [zeros], axis=0)

    for g in range(LONG // WIN):
        if g < FULL // WIN:
            copies[g].wait()
        elif g == FULL // WIN:
            for copy in copies[g:]:
                copy.wait()
        flat = [
            lax.dot_general(
                pick, slab(g * WIN + k), (((1,), (1,)), ((), ())), preferred_element_type=jnp.float32
            ).astype(jnp.bfloat16)
            for k in range(WIN)
        ]
        for t in range(devices // WIN):
            mixed = jnp.concatenate([f[t * WIN : (t + 1) * WIN] for f in flat], axis=0)
            done = jnp.dot(turn, mixed, preferred_element_type=jnp.float32).astype(jnp.bfloat16)
            done = done.reshape(WIN, WIN, LANES)
            wire[g, t * WIN : (t + 1) * WIN] = done
        pltpu.make_async_copy(wire.at[g], out.at[:, g * WIN : (g + 1) * WIN], sent.at[g]).start()
    for g in range(LONG // WIN):
        pltpu.make_async_copy(wire.at[g], out.at[:, g * WIN : (g + 1) * WIN], sent.at[g]).wait()


def pack_call(own, q_own, source):
    height, _, depth = source.shape
    source = pltpu.with_memory_space_constraint(source, pltpu.HBM)
    return pl.pallas_call(
        functools.partial(pack, own, q_own),
        out_shape=pltpu.HBM((depth // q_own, LONG, LANES), jnp.bfloat16),
        in_specs=[HBM],
        out_specs=HBM,
        scratch_shapes=[
            pltpu.VMEM(source.shape, jnp.bfloat16),
            pltpu.VMEM((LONG // WIN, depth // q_own, WIN, LANES), jnp.bfloat16),
            pltpu.SemaphoreType.DMA((-(-height // WIN),)),
            pltpu.SemaphoreType.DMA((LONG // WIN,)),
        ],
        compiler_params=pltpu.CompilerParams(vmem_limit_bytes=20 * 2**20),
        cost_estimate=pl.CostEstimate(flops=5 * 10**9, bytes_accessed=10**7, transcendentals=0),
        name="pack",
    )(source)


def dress(own, last, pieces, win, cols, sel, *rest):
    if last:
        core, before, _, whole, mine, theirs, held, x, top, stage, hsem, sem, fock, fsem = rest
    else:
        whole, kept, held, x, top, stage, hsem, sem, fock, fsem = rest
    rows = x.shape[0]
    blocks = x.shape[2] // CP
    width = stage.shape[1] // blocks
    side = width - LANES
    per = rows // blocks
    deep, tall = per * RP, per * SH

    def come(m):
        part = pl.ds(m * per * blocks, per * blocks)
        return pltpu.make_async_copy(pieces.at[part], held.at[part], hsem.at[m])

    def leave(m):
        part = pl.ds(m * tall, tall)
        return pltpu.make_async_copy(stage.at[part], whole.at[own, part], sem.at[m])

    def carried(m):
        if last:
            return pltpu.make_async_copy(before.at[m], fock.at[m], fsem.at[m])
        return pltpu.make_async_copy(fock.at[m], kept.at[m], fsem.at[m])

    for m in range(blocks):
        come(m).start()
    if last:
        for m in range(blocks):
            carried(m).start()
    for c in range(blocks):
        x[:, :, c * CP + width : (c + 1) * CP] = jnp.zeros((rows, RP, CP - width), jnp.bfloat16)
    x[:, FULL:, :] = jnp.zeros((rows, RP - FULL, blocks * CP), jnp.bfloat16)

    def place(r, carry):
        for c in range(blocks):
            at = r * blocks + c
            lane = c * CP
            x[r, :FULL, lane : lane + LANES] = held[at, :FULL, :]
            x[r, FULL:SH, lane : lane + LANES] = held[at, FULL + TALL :, :]
            for i in range(3):
                x[r, i * TALL : (i + 1) * TALL, lane + LANES : lane + width] = held[
                    at, FULL : FULL + TALL, i * side : (i + 1) * side
                ]
        return carry

    for m in range(blocks):
        come(m).wait()
        lax.fori_loop(m * per, (m + 1) * per, place, 0)
    flat = x.reshape(rows * RP, blocks * CP)
    shift = jnp.dot(win[...], flat[...], preferred_element_type=jnp.float32)
    for r in range(rows):
        at = slice(r * RP, r * RP + WIN)
        fixed = flat[at, :].astype(jnp.float32) - shift[r * WIN : (r + 1) * WIN]
        flat[at, :] = fixed.astype(jnp.bfloat16)
    g = jnp.dot(flat[...], sel[...], preferred_element_type=jnp.float32).astype(jnp.bfloat16)
    inner = jnp.concatenate([g[r * RP : r * RP + WIN, :] for r in range(rows)], axis=0)
    here = lax.broadcasted_iota(jnp.int32, inner.shape, 0)
    there = lax.broadcasted_iota(jnp.int32, inner.shape, 1)
    weight = 2.0 * jnp.sum(jnp.where(here == there, inner.astype(jnp.float32), 0.0))
    for m in range(blocks):
        at = slice(m * deep, (m + 1) * deep)
        extra = jnp.dot(g[at], cols[...], preferred_element_type=jnp.float32)
        new = (flat[at, :].astype(jnp.float32) + extra).astype(jnp.bfloat16)
        flat[at, :] = new
        for r in range(per):
            for c in range(blocks):
                block = new[r * RP : r * RP + SH, c * CP : c * CP + width]
                down = m * tall + r * SH
                stage[down : down + SH, c * width : (c + 1) * width] = block
            to = (m * per + r) * WIN
            top[to : to + WIN, :] = new[r * RP : r * RP + WIN, :]
        leave(m).start()

    def wired(target, at, block):
        target[at, :FULL, :] = block[:FULL, :LANES]
        target[at, FULL + TALL :, :] = block[FULL:, :LANES]
        for i in range(3):
            target[at, FULL : FULL + TALL, i * side : (i + 1) * side] = block[
                i * TALL : (i + 1) * TALL, LANES:
            ]
        target[at, FULL : FULL + TALL, 3 * side :] = jnp.zeros(
            (TALL, LANES - 3 * side), jnp.bfloat16
        )

    for m in range(blocks):
        at = slice(m * deep, (m + 1) * deep)
        swapped = jnp.dot(g[at], top[...], preferred_element_type=jnp.float32)
        total = weight * flat[at, :].astype(jnp.float32) - swapped
        if not last:
            fock[m] = total.astype(jnp.bfloat16)
            carried(m).start()
            continue
        odd = core[0] == 1
        carried(m).wait()
        total = (total + fock[m].astype(jnp.float32)).astype(jnp.bfloat16)
        for r in range(per):
            for h in range(blocks // 2):
                pair = [
                    total[r * RP : r * RP + SH, c * CP : c * CP + width] for c in (2 * h, 2 * h + 1)
                ]
                to = (m * per + r) * (blocks // 2) + h
                wired(mine, to, jnp.where(odd, pair[1], pair[0]))
                wired(theirs, to, jnp.where(odd, pair[0], pair[1]))
    for m in range(blocks):
        leave(m).wait()
        if not last:
            carried(m).wait()


def dress_call(own, q_own, shape, pieces, win, cols, sel, core=None, before=None, whole=None):
    last = before is not None
    rows, blocks, _ = shape
    norb = rows * SH
    pieces = pltpu.with_memory_space_constraint(pieces, pltpu.HBM)
    half = pltpu.VMEM((rows * blocks // 2, LONG, LANES), jnp.bfloat16)
    split = (blocks, rows // blocks * RP, blocks * CP)
    whole_shape = pltpu.HBM((q_own, norb, norb), jnp.bfloat16)
    if last:
        before = pltpu.with_memory_space_constraint(before, pltpu.HBM)
        args = (pieces, win, cols, sel, core, before, whole)
        in_specs = [HBM, VMEM, VMEM, VMEM, pl.BlockSpec(memory_space=pltpu.SMEM), HBM, HBM]
        out_shape, out_specs = (whole_shape, half, half), (HBM, VMEM, VMEM)
    else:
        args = (pieces, win, cols, sel)
        in_specs = [HBM, VMEM, VMEM, VMEM]
        out_shape = (whole_shape, pltpu.HBM(split, jnp.bfloat16))
        out_specs = (HBM, HBM)
    sem = pltpu.SemaphoreType.DMA((blocks,))
    return pl.pallas_call(
        functools.partial(dress, own, last),
        out_shape=out_shape,
        in_specs=in_specs,
        out_specs=out_specs,
        input_output_aliases={6: 0} if last else {},
        scratch_shapes=[
            pltpu.VMEM(pieces.shape, jnp.bfloat16),
            pltpu.VMEM((rows, RP, blocks * CP), jnp.bfloat16),
            pltpu.VMEM((rows * WIN, blocks * CP), jnp.bfloat16),
            pltpu.VMEM((norb, norb), jnp.bfloat16),
            sem,
            sem,
            pltpu.VMEM(split, jnp.bfloat16),
            sem,
        ],
        compiler_params=pltpu.CompilerParams(vmem_limit_bytes=48 * 2**20),
        cost_estimate=pl.CostEstimate(flops=10**10, bytes_accessed=10**7, transcendentals=0),
        name="dress_last" if last else "dress_first",
    )(*args)


def finish(own, other, fock):
    width = fock.shape[1]
    side = width - LANES
    total = own[...].astype(jnp.float32) + other[...].astype(jnp.float32)
    fock[:FULL, :LANES] = total[:FULL]
    fock[FULL:, :LANES] = total[FULL + TALL :]
    for i in range(3):
        fock[i * TALL : (i + 1) * TALL, LANES:] = total[
            FULL : FULL + TALL, i * side : (i + 1) * side
        ]


def finish_call(own, other, width):
    own = pltpu.with_memory_space_constraint(own, pltpu.VMEM)
    other = pltpu.with_memory_space_constraint(other, pltpu.VMEM)
    return pl.pallas_call(
        finish,
        out_shape=jax.ShapeDtypeStruct((SH, width), jnp.float32),
        in_specs=[VMEM] * 2,
        out_specs=VMEM,
        name="finish",
    )(own, other)


def fold(amp, out):
    tall, wide = out.shape[0], amp.shape[1]
    out[...] = jnp.zeros_like(out)
    for i in range(amp.shape[0] // tall):
        out[:, i * FULL : i * FULL + wide] = amp[i * tall : (i + 1) * tall, :]


def fold_call(amp):
    return pl.pallas_call(
        fold,
        out_shape=jax.ShapeDtypeStruct((amp.shape[0] // 3, LANES), amp.dtype),
        in_specs=[VMEM],
        out_specs=VMEM,
        name="fold",
    )(amp)


def join(here, *refs):
    count, out = len(refs) - 1, refs[-1]
    tall, wide = refs[0].shape[0], out.shape[2]
    for step in range(count):
        to = lax.rem(here[0] + step, count)
        for i in range(out.shape[1] // tall):
            out[to, i * tall : (i + 1) * tall, :] = refs[step][:, i * FULL : i * FULL + wide]


def join_call(here, parts, shape):
    return pl.pallas_call(
        join,
        out_shape=jax.ShapeDtypeStruct((len(parts), *shape), parts[0].dtype),
        in_specs=[pl.BlockSpec(memory_space=pltpu.SMEM)] + [VMEM] * len(parts),
        out_specs=VMEM,
        name="join",
    )(here, *parts)


def tables(amp, blocks):
    groups = amp.shape[0]
    cut = amp.reshape(groups, groups, OG, SH - OG)
    cut = jnp.pad(cut, ((0, 0), (0, 0), (0, WIN - OG), (OG, 0))).reshape(groups, groups * WIN, SH)
    win = jnp.pad(cut, ((0, 0), (0, 0), (0, RP - SH)))
    win = jnp.transpose(win, (1, 0, 2)).reshape(groups * WIN, groups * RP)
    per = groups // blocks
    cols = jnp.transpose(cut, (1, 0, 2)).reshape(groups * WIN, blocks, per * SH)
    cols = jnp.pad(cols, ((0, 0), (0, 0), (0, CP - per * SH))).reshape(groups * WIN, blocks * CP)
    at = lax.broadcasted_iota(jnp.int32, (blocks * CP, groups * WIN), 0)
    to = lax.broadcasted_iota(jnp.int32, (blocks * CP, groups * WIN), 1)
    inside = at % CP
    group = at // CP * per + inside // SH
    hit = (inside < per * SH) & (to // WIN == group) & (to % WIN == inside % SH) & (inside % SH < OG)
    return win, cols, hit.astype(jnp.bfloat16)


ROW = ("row_0", "row_1")
COL = ("col_0", "col_1")
ALL = (*ROW, *COL)


def swap(array, axis):
    return lax.all_to_all(array, axis, split_axis=0, concat_axis=0, tiled=True)


def all_of(array, axis):
    count = lax.axis_size(axis)
    here = lax.axis_index(axis)
    folded = fold_call(array)
    found = [folded]
    for step in range(1, count):
        pairs = [((to + step) % count, to) for to in range(count)]
        found.append(lax.ppermute(folded, axis, pairs))
    return join_call(here.astype(jnp.int32).reshape(1), found, array.shape)


def step(chol, amplitudes):
    q_local, _, col_width = chol.shape
    shape = (lax.axis_size(ROW), lax.axis_size(COL), col_width)
    q_own = q_local // lax.axis_size(ALL)
    source = jnp.transpose(chol, (1, 2, 0))
    sent, amplitudes = lax.optimization_barrier((pack_call(0, q_own, source), amplitudes))
    first = swap(sent, ALL)
    amp = all_of(amplitudes, ROW)
    win, into, sel = tables(amp, shape[1])
    second = swap(pack_call(1, q_own, source), ALL)
    core = lax.axis_index("col_1").astype(jnp.int32).reshape(1)
    whole, part = dress_call(0, q_own, shape, first, win, into, sel)
    whole, mine, theirs = dress_call(1, q_own, shape, second, win, into, sel, core, part, whole)
    came = lax.ppermute(theirs, "col_1", ((0, 1), (1, 0)))
    fock = (mine.astype(jnp.float32) + came.astype(jnp.float32)).astype(jnp.bfloat16)
    fock = swap(fock, (*ROW, "col_0"))
    fock = jnp.sum(fock.astype(jnp.float32), axis=0).astype(jnp.bfloat16)
    other = lax.ppermute(fock, "pb", ((0, 1), (1, 0)))
    return whole, finish_call(fock, other, col_width)


def solution(mesh):
    finer = Mesh(
        mesh.devices.reshape(mesh.shape["pb"], 4, 4, mesh.shape["col"] // 2, 2),
        ("pb", *ALL),
    )
    placed = (P("pb", ROW, COL), P(None, ROW))
    return jax.shard_map(
        step,
        mesh=finer,
        in_specs=placed,
        out_specs=(P(("pb", *ALL), None, None), P(ROW, COL)),
        check_vma=False,
    )
```

```python
import functools

import jax
import jax.numpy as jnp
from jax import lax
from jax.experimental import pallas as pl
from jax.experimental.pallas import tpu as pltpu
from jax.sharding import Mesh
from jax.sharding import PartitionSpec as P

OG, SH = 9, 84
RP, CP, WIN = 96, 384, 16
FULL, LANES, TALL, LONG = 80, 256, 28, 112
VMEM = pl.BlockSpec(memory_space=pltpu.VMEM)
HBM = pl.BlockSpec(memory_space=pltpu.HBM)


def hot(condition):
    return jnp.where(condition, 1.0, 0.0).astype(jnp.bfloat16)


def pack(own, q_own, source, out, held, wire, sem, sent):
    height, width, depth = held.shape
    rest = width - LANES
    devices = depth // q_own
    parts = [(pl.ds(at, WIN), pl.ds(0, LANES)) for at in range(0, FULL, WIN)]
    parts += [(pl.ds(0, height), pl.ds(LANES, rest)), (pl.ds(FULL, height - FULL), pl.ds(0, LANES))]
    copies = [
        pltpu.make_async_copy(source.at[part], held.at[part], sem.at[k])
        for k, part in enumerate(parts)
    ]
    for copy in copies:
        copy.start()
    row = lax.broadcasted_iota(jnp.int32, (devices, depth), 0)
    col = lax.broadcasted_iota(jnp.int32, (devices, depth), 1)
    pick = hot(col == row * q_own + own)
    row = lax.broadcasted_iota(jnp.int32, (LANES, LANES), 0)
    col = lax.broadcasted_iota(jnp.int32, (LANES, LANES), 1)
    turn = hot((row // WIN == col % WIN) & (row % WIN == col // WIN))
    zeros = jnp.zeros((LANES - 3 * rest, depth), jnp.bfloat16)

    def slab(k):
        if k < FULL:
            return held[k, :LANES, :]
        k -= FULL
        if k >= TALL:
            return held[FULL + k - TALL, :LANES, :]
        parts = [held[i * TALL + k, LANES:, :] for i in range(3)]
        return jnp.concatenate(parts + [zeros], axis=0)

    for g in range(LONG // WIN):
        if g < FULL // WIN:
            copies[g].wait()
        elif g == FULL // WIN:
            for copy in copies[g:]:
                copy.wait()
        flat = [
            lax.dot_general(
                pick, slab(g * WIN + k), (((1,), (1,)), ((), ())), preferred_element_type=jnp.float32
            ).astype(jnp.bfloat16)
            for k in range(WIN)
        ]
        for t in range(devices // WIN):
            mixed = jnp.concatenate([f[t * WIN : (t + 1) * WIN] for f in flat], axis=0)
            done = jnp.dot(turn, mixed, preferred_element_type=jnp.float32).astype(jnp.bfloat16)
            done = done.reshape(WIN, WIN, LANES)
            wire[g, t * WIN : (t + 1) * WIN] = done
        pltpu.make_async_copy(wire.at[g], out.at[:, g * WIN : (g + 1) * WIN], sent.at[g]).start()
    for g in range(LONG // WIN):
        pltpu.make_async_copy(wire.at[g], out.at[:, g * WIN : (g + 1) * WIN], sent.at[g]).wait()


def pack_call(own, q_own, source):
    _, _, depth = source.shape
    source = pltpu.with_memory_space_constraint(source, pltpu.HBM)
    return pl.pallas_call(
        functools.partial(pack, own, q_own),
        out_shape=pltpu.HBM((depth // q_own, LONG, LANES), jnp.bfloat16),
        in_specs=[HBM],
        out_specs=HBM,
        scratch_shapes=[
            pltpu.VMEM(source.shape, jnp.bfloat16),
            pltpu.VMEM((LONG // WIN, depth // q_own, WIN, LANES), jnp.bfloat16),
            pltpu.SemaphoreType.DMA((FULL // WIN + 2,)),
            pltpu.SemaphoreType.DMA((LONG // WIN,)),
        ],
        compiler_params=pltpu.CompilerParams(vmem_limit_bytes=20 * 2**20),
        cost_estimate=pl.CostEstimate(flops=5 * 10**9, bytes_accessed=10**7, transcendentals=0),
        name="pack",
    )(source)


def dress(own, last, pieces, win, cols, sel, *rest):
    if last:
        core, before, _, whole, mine, theirs, held, x, top, stage, hsem, sem, fock, fsem = rest
    else:
        whole, kept, held, x, top, stage, hsem, sem, fock, fsem = rest
    rows = x.shape[0]
    blocks = x.shape[2] // CP
    width = stage.shape[1] // blocks
    side = width - LANES
    per = rows // blocks
    deep, tall = per * RP, per * SH

    def come(m):
        part = pl.ds(m * per * blocks, per * blocks)
        return pltpu.make_async_copy(pieces.at[part], held.at[part], hsem.at[m])

    def leave(m):
        part = pl.ds(m * tall, tall)
        return pltpu.make_async_copy(stage.at[part], whole.at[own, part], sem.at[m])

    def carried(m):
        if last:
            return pltpu.make_async_copy(before.at[m], fock.at[m], fsem.at[m])
        return pltpu.make_async_copy(fock.at[m], kept.at[m], fsem.at[m])

    for m in range(blocks):
        come(m).start()
    if last:
        for m in range(blocks):
            carried(m).start()
    for c in range(blocks):
        x[:, :, c * CP + width : (c + 1) * CP] = jnp.zeros((rows, RP, CP - width), jnp.bfloat16)
    x[:, FULL:, :] = jnp.zeros((rows, RP - FULL, blocks * CP), jnp.bfloat16)

    def place(r, carry):
        for c in range(blocks):
            at = r * blocks + c
            lane = c * CP
            x[r, :FULL, lane : lane + LANES] = held[at, :FULL, :]
            x[r, FULL:SH, lane : lane + LANES] = held[at, FULL + TALL :, :]
            for i in range(3):
                x[r, i * TALL : (i + 1) * TALL, lane + LANES : lane + width] = held[
                    at, FULL : FULL + TALL, i * side : (i + 1) * side
                ]
        return carry

    for m in range(blocks):
        come(m).wait()
        lax.fori_loop(m * per, (m + 1) * per, place, 0)
    flat = x.reshape(rows * RP, blocks * CP)
    shift = jnp.dot(win[...], flat[...], preferred_element_type=jnp.float32)
    for r in range(rows):
        at = slice(r * RP, r * RP + WIN)
        fixed = flat[at, :].astype(jnp.float32) - shift[r * WIN : (r + 1) * WIN]
        flat[at, :] = fixed.astype(jnp.bfloat16)
    g = jnp.dot(flat[...], sel[...], preferred_element_type=jnp.float32).astype(jnp.bfloat16)
    inner = jnp.concatenate([g[r * RP : r * RP + WIN, :] for r in range(rows)], axis=0)
    here = lax.broadcasted_iota(jnp.int32, inner.shape, 0)
    there = lax.broadcasted_iota(jnp.int32, inner.shape, 1)
    weight = 2.0 * jnp.sum(jnp.where(here == there, inner.astype(jnp.float32), 0.0))
    for m in range(blocks):
        at = slice(m * deep, (m + 1) * deep)
        extra = jnp.dot(g[at], cols[...], preferred_element_type=jnp.float32)
        new = (flat[at, :].astype(jnp.float32) + extra).astype(jnp.bfloat16)
        flat[at, :] = new
        for r in range(per):
            for c in range(blocks):
                block = new[r * RP : r * RP + SH, c * CP : c * CP + width]
                down = m * tall + r * SH
                stage[down : down + SH, c * width : (c + 1) * width] = block
            to = (m * per + r) * WIN
            top[to : to + WIN, :] = new[r * RP : r * RP + WIN, :]
        leave(m).start()

    def wired(target, at, block):
        target[at, :FULL, :] = block[:FULL, :LANES]
        target[at, FULL + TALL :, :] = block[FULL:, :LANES]
        for i in range(3):
            target[at, FULL : FULL + TALL, i * side : (i + 1) * side] = block[
                i * TALL : (i + 1) * TALL, LANES:
            ]
        target[at, FULL : FULL + TALL, 3 * side :] = jnp.zeros(
            (TALL, LANES - 3 * side), jnp.bfloat16
        )

    for m in range(blocks):
        at = slice(m * deep, (m + 1) * deep)
        swapped = jnp.dot(g[at], top[...], preferred_element_type=jnp.float32)
        total = weight * flat[at, :].astype(jnp.float32) - swapped
        if not last:
            fock[m] = total.astype(jnp.bfloat16)
            carried(m).start()
            continue
        odd = core[0] == 1
        carried(m).wait()
        total = (total + fock[m].astype(jnp.float32)).astype(jnp.bfloat16)
        for r in range(per):
            for h in range(blocks // 2):
                pair = [
                    total[r * RP : r * RP + SH, c * CP : c * CP + width] for c in (2 * h, 2 * h + 1)
                ]
                to = (m * per + r) * (blocks // 2) + h
                wired(mine, to, jnp.where(odd, pair[1], pair[0]))
                wired(theirs, to, jnp.where(odd, pair[0], pair[1]))
    for m in range(blocks):
        leave(m).wait()
        if not last:
            carried(m).wait()


def dress_call(own, q_own, shape, pieces, win, cols, sel, core=None, before=None, whole=None):
    last = before is not None
    rows, blocks, _ = shape
    norb = rows * SH
    pieces = pltpu.with_memory_space_constraint(pieces, pltpu.HBM)
    half = pltpu.VMEM((rows * blocks // 2, LONG, LANES), jnp.bfloat16)
    split = (blocks, rows // blocks * RP, blocks * CP)
    whole_shape = pltpu.HBM((q_own, norb, norb), jnp.bfloat16)
    if last:
        before = pltpu.with_memory_space_constraint(before, pltpu.HBM)
        args = (pieces, win, cols, sel, core, before, whole)
        in_specs = [HBM, VMEM, VMEM, VMEM, pl.BlockSpec(memory_space=pltpu.SMEM), HBM, HBM]
        out_shape, out_specs = (whole_shape, half, half), (HBM, VMEM, VMEM)
    else:
        args = (pieces, win, cols, sel)
        in_specs = [HBM, VMEM, VMEM, VMEM]
        out_shape = (whole_shape, pltpu.HBM(split, jnp.bfloat16))
        out_specs = (HBM, HBM)
    sem = pltpu.SemaphoreType.DMA((blocks,))
    return pl.pallas_call(
        functools.partial(dress, own, last),
        out_shape=out_shape,
        in_specs=in_specs,
        out_specs=out_specs,
        input_output_aliases={6: 0} if last else {},
        scratch_shapes=[
            pltpu.VMEM(pieces.shape, jnp.bfloat16),
            pltpu.VMEM((rows, RP, blocks * CP), jnp.bfloat16),
            pltpu.VMEM((rows * WIN, blocks * CP), jnp.bfloat16),
            pltpu.VMEM((norb, norb), jnp.bfloat16),
            sem,
            sem,
            pltpu.VMEM(split, jnp.bfloat16),
            sem,
        ],
        compiler_params=pltpu.CompilerParams(vmem_limit_bytes=48 * 2**20),
        cost_estimate=pl.CostEstimate(flops=10**10, bytes_accessed=10**7, transcendentals=0),
        name="dress_last" if last else "dress_first",
    )(*args)


def finish(own, other, fock):
    width = fock.shape[1]
    side = width - LANES
    total = own[...].astype(jnp.float32) + other[...].astype(jnp.float32)
    fock[:FULL, :LANES] = total[:FULL]
    fock[FULL:, :LANES] = total[FULL + TALL :]
    for i in range(3):
        fock[i * TALL : (i + 1) * TALL, LANES:] = total[
            FULL : FULL + TALL, i * side : (i + 1) * side
        ]


def finish_call(own, other, width):
    own = pltpu.with_memory_space_constraint(own, pltpu.VMEM)
    other = pltpu.with_memory_space_constraint(other, pltpu.VMEM)
    return pl.pallas_call(
        finish,
        out_shape=jax.ShapeDtypeStruct((SH, width), jnp.float32),
        in_specs=[VMEM] * 2,
        out_specs=VMEM,
        name="finish",
    )(own, other)


def fold(amp, out):
    tall, wide = out.shape[0], amp.shape[1]
    out[...] = jnp.zeros_like(out)
    for i in range(amp.shape[0] // tall):
        out[:, i * FULL : i * FULL + wide] = amp[i * tall : (i + 1) * tall, :]


def fold_call(amp):
    return pl.pallas_call(
        fold,
        out_shape=jax.ShapeDtypeStruct((amp.shape[0] // 3, LANES), amp.dtype),
        in_specs=[VMEM],
        out_specs=VMEM,
        name="fold",
    )(amp)


def join(here, *refs):
    count, out = len(refs) - 1, refs[-1]
    tall, wide = refs[0].shape[0], out.shape[2]
    for step in range(count):
        to = lax.rem(here[0] + step, count)
        for i in range(out.shape[1] // tall):
            out[to, i * tall : (i + 1) * tall, :] = refs[step][:, i * FULL : i * FULL + wide]


def join_call(here, parts, shape):
    return pl.pallas_call(
        join,
        out_shape=jax.ShapeDtypeStruct((len(parts), *shape), parts[0].dtype),
        in_specs=[pl.BlockSpec(memory_space=pltpu.SMEM)] + [VMEM] * len(parts),
        out_specs=VMEM,
        name="join",
    )(here, *parts)


def tables(amp, blocks):
    groups = amp.shape[0]
    cut = amp.reshape(groups, groups, OG, SH - OG)
    cut = jnp.pad(cut, ((0, 0), (0, 0), (0, WIN - OG), (OG, 0))).reshape(groups, groups * WIN, SH)
    win = jnp.pad(cut, ((0, 0), (0, 0), (0, RP - SH)))
    win = jnp.transpose(win, (1, 0, 2)).reshape(groups * WIN, groups * RP)
    per = groups // blocks
    cols = jnp.transpose(cut, (1, 0, 2)).reshape(groups * WIN, blocks, per * SH)
    cols = jnp.pad(cols, ((0, 0), (0, 0), (0, CP - per * SH))).reshape(groups * WIN, blocks * CP)
    at = lax.broadcasted_iota(jnp.int32, (blocks * CP, groups * WIN), 0)
    to = lax.broadcasted_iota(jnp.int32, (blocks * CP, groups * WIN), 1)
    inside = at % CP
    group = at // CP * per + inside // SH
    hit = (inside < per * SH) & (to // WIN == group) & (to % WIN == inside % SH) & (inside % SH < OG)
    return win, cols, hit.astype(jnp.bfloat16)


ROW = ("row_0", "row_1")
COL = ("col_0", "col_1")
ALL = (*ROW, *COL)


def swap(array, axis):
    return lax.all_to_all(array, axis, split_axis=0, concat_axis=0, tiled=True)


def all_of(array, axis):
    count = lax.axis_size(axis)
    here = lax.axis_index(axis)
    folded = fold_call(array)
    found = [folded]
    for step in range(1, count):
        pairs = [((to + step) % count, to) for to in range(count)]
        found.append(lax.ppermute(folded, axis, pairs))
    return join_call(here.astype(jnp.int32).reshape(1), found, array.shape)


def step(chol, amplitudes):
    q_local, _, col_width = chol.shape
    shape = (lax.axis_size(ROW), lax.axis_size(COL), col_width)
    q_own = q_local // lax.axis_size(ALL)
    source = jnp.transpose(chol, (1, 2, 0))
    sent, amplitudes = lax.optimization_barrier((pack_call(0, q_own, source), amplitudes))
    first = swap(sent, ALL)
    amp = all_of(amplitudes, ROW)
    win, into, sel = tables(amp, shape[1])
    second = swap(pack_call(1, q_own, source), ALL)
    core = lax.axis_index("col_1").astype(jnp.int32).reshape(1)
    whole, part = dress_call(0, q_own, shape, first, win, into, sel)
    whole, mine, theirs = dress_call(1, q_own, shape, second, win, into, sel, core, part, whole)
    came = lax.ppermute(theirs, "col_1", ((0, 1), (1, 0)))
    fock = (mine.astype(jnp.float32) + came.astype(jnp.float32)).astype(jnp.bfloat16)
    fock = swap(fock, (*ROW, "col_0"))
    fock = jnp.sum(fock.astype(jnp.float32), axis=0).astype(jnp.bfloat16)
    other = lax.ppermute(fock, "pb", ((0, 1), (1, 0)))
    return whole, finish_call(fock, other, col_width)


def solution(mesh):
    finer = Mesh(
        mesh.devices.reshape(mesh.shape["pb"], 4, 4, mesh.shape["col"] // 2, 2),
        ("pb", *ALL),
    )
    placed = (P("pb", ROW, COL), P(None, ROW))
    return jax.shard_map(
        step,
        mesh=finer,
        in_specs=placed,
        out_specs=(P(("pb", *ALL), None, None), P(ROW, COL)),
        check_vma=False,
    )
```
